32 devices in a mesh: loader: 32 (over z, y, x, core).
Axes of the slice: x: 2, y: 2, z: 4, core: 2. Of those that a mesh axis runs over, the one named last changes fastest.
Arguments:
- image_embed: bfloat16 [49152, 512], P('loader'), may hold values from -600 to 600
- text_embed: bfloat16 [49152, 512], P('loader'), may hold values from -600 to 600
- keep_mask: int32 [49152], P('loader'), may hold values from 0 to 1
Outputs:
- packed_pairs: bfloat16 [49152, 1024], P('loader')
- pair_scores: float32 [49152], P('loader')
The draws below stay inside these ranges and needn't reach their ends.
All inputs are finite; a program needn't handle non-finite values.
Results may differ from the reference program's by a relative error of at most 0.002.
Values may be sent and summed in bfloat16 or wider, within the bound.
No kernel may reach another device: no remote copies, remote signals or barrier semaphores. Data moves between devices by JAX's collectives and lax.ppermute only.
A program may use at most 64 MiB of HBM per device.

```python
import jax
import jax.numpy as jnp
from jax import lax

D = 512
ROWS = 1536
N_LOADER = 32


def embed_pair(key):
    total_rows = ROWS * N_LOADER
    core_key, noise_key, row_key, column_key = jax.random.split(jax.random.fold_in(key, 7), 4)
    core = jnp.clip(jax.random.normal(core_key, (total_rows, D), jnp.float32), -4.0, 4.0)
    noise = jnp.clip(jax.random.normal(noise_key, (total_rows, D), jnp.float32), -4.0, 4.0)
    partner = 0.6 * core + 0.8 * noise
    row_scales = jnp.exp(jax.random.uniform(row_key, (2, total_rows, 1), jnp.float32, 0.0, 2.3))
    column_scales = jnp.exp(jax.random.uniform(column_key, (2, 1, D), jnp.float32, 0.0, 2.3))
    return (core * row_scales[0] * column_scales[0], partner * row_scales[1] * column_scales[1])


def draw_image_embed(key, part):
    return embed_pair(key)[0].astype(jnp.bfloat16)


def draw_text_embed(key, part):
    return embed_pair(key)[1].astype(jnp.bfloat16)


def draw_keep_mask(key, part):
    count_key, extra_key, full_key, order_key = jax.random.split(jax.random.fold_in(key, 19), 4)
    draw_one = jax.random.randint(count_key, (N_LOADER,), 0, ROWS + 1)
    draw_two = jax.random.randint(extra_key, (N_LOADER,), 0, ROWS + 1)
    kept_counts = (draw_one + draw_one * draw_two // ROWS) // 2
    chosen = jax.random.randint(full_key, (), 0, N_LOADER)
    kept_counts = jnp.where(jnp.arange(N_LOADER) == chosen, ROWS, kept_counts)
    orders = jax.vmap(lambda shard_key: jax.random.permutation(shard_key, ROWS))(jax.random.split(order_key, N_LOADER))
    return (orders < kept_counts[:, None]).astype(jnp.int32).reshape(ROWS * N_LOADER)


def setup_inputs(seed: int = 0) -> dict:
    arg_keys = jax.random.split(jax.random.key(seed), 4)
    image_embed = draw_image_embed(jax.random.fold_in(arg_keys[3], 71), 0)
    text_embed = draw_text_embed(jax.random.fold_in(arg_keys[3], 71), 0)
    keep_mask = draw_keep_mask(jax.random.fold_in(arg_keys[3], 71), 0)
    return {"image_embed": image_embed, "text_embed": text_embed, "keep_mask": keep_mask}


epsilon = 1e-06

def unit_rows(embedding):
    values = embedding.astype(jnp.float32)
    scale = lax.rsqrt(lax.optimization_barrier(jnp.mean(values * values, axis=1, keepdims=True)) + epsilon)
    return (values * scale).astype(jnp.bfloat16)

def pair_score(packed):
    halves = packed.shape[1] // 2
    left_part = packed[:, :halves].astype(jnp.float32)
    right_part = packed[:, halves:].astype(jnp.float32)
    return lax.optimization_barrier(jnp.sum(left_part * right_part, axis=1)) / halves

def reference(image_embed, text_embed, keep_mask):
    payload = jnp.concatenate([unit_rows(image_embed), unit_rows(text_embed)], axis=1)
    row_ranks = (jnp.cumsum(keep_mask) - keep_mask).astype(jnp.int32)
    total_rows = keep_mask.shape[0]
    destination = jnp.where(keep_mask == 1, row_ranks, total_rows).astype(jnp.int32)
    packed = jnp.zeros_like(payload).at[destination].set(payload, mode='drop')
    return (packed, pair_score(packed))
```

```python
import functools

import jax
import jax.numpy as jnp
from jax import lax
from jax.experimental import pallas as pl
from jax.experimental.pallas import tpu as pltpu
from jax.sharding import PartitionSpec as P

epsilon = 1e-06
TILE = 16
BLOCK = 256
WINDOWS = ((768, 704), (1024, 1024, 256))

SMEM = pl.BlockSpec(memory_space=pltpu.SMEM)
VMEM = pl.BlockSpec(memory_space=pltpu.VMEM)


def group_of(devices):
    return 2 ** (devices.bit_length() // 2)


def before(counts_ref, index):
    return lax.fori_loop(0, index, lambda s, total: total + counts_ref[s], jnp.int32(0))


def dealt(rank, member, group):
    turn = group * TILE
    return rank // turn * TILE + jnp.clip(rank % turn - member * TILE, 0, TILE)


def pack_kernel(group, counts_ref, sums_ref, mask_ref, x_ref, *rest):
    outs, packed, ahead = rest[:group], rest[group], rest[group + 1]
    rows, width = x_ref.shape
    blocks = rows // BLOCK
    me = lax.axis_index("loader")
    member = me % group
    packed[...] = jnp.zeros_like(packed)
    r = lax.broadcasted_iota(jnp.int32, (BLOCK, BLOCK), 0)
    c = lax.broadcasted_iota(jnp.int32, (BLOCK, BLOCK), 1)
    triangle = (r < c).astype(jnp.float32).astype(jnp.bfloat16)
    marks = mask_ref[...].astype(jnp.float32).astype(jnp.bfloat16)
    ahead[...] = jnp.dot(marks, triangle, preferred_element_type=jnp.float32).astype(jnp.int32)

    def step(b, base):
        values = x_ref[pl.ds(pl.multiple_of(b * BLOCK, BLOCK), BLOCK), :].astype(jnp.float32)
        scale = lax.rsqrt(jnp.sum(values * values, axis=1, keepdims=True) / width + epsilon)
        unit = (values * scale).astype(jnp.bfloat16)
        kept = mask_ref[pl.ds(b, 1), :] == 1
        into = base % BLOCK
        slot = jnp.where(kept, ahead[pl.ds(b, 1), :] + into, -1)

        def put(first, block):
            chosen = (slot - first == r).astype(jnp.float32).astype(jnp.bfloat16)
            part = jnp.dot(chosen, unit, preferred_element_type=jnp.float32).astype(jnp.bfloat16)
            for e in range(BLOCK // TILE):
                at = block * (BLOCK // TILE // group) + e // group
                where = pl.ds(pl.multiple_of(at * TILE, TILE), TILE)
                packed[e % group, where, :] += part[e * TILE : (e + 1) * TILE]

        count = sums_ref[b]

        @pl.when(count > 0)
        def _():
            put(0, base // BLOCK)

        @pl.when(into + count > BLOCK)
        def _():
            put(BLOCK, (base // BLOCK + 1) % blocks)

        return (base + count) % rows

    lax.fori_loop(0, blocks, step, before(counts_ref, me) % rows)
    for k in range(group):
        outs[k][...] = packed[jnp.bitwise_xor(member, k)]


def copy_rows(low, high, source, source_tile, target, target_tile):
    width = target.shape[-1]

    def tile(t, _):
        row = t * TILE + lax.broadcasted_iota(jnp.int32, (TILE, width), 0)
        inside = (row >= low) & (row < high)
        at = pl.ds(pl.multiple_of(target_tile(t) * TILE, TILE), TILE)
        value = source[pl.ds(pl.multiple_of(source_tile(t) * TILE, TILE), TILE), :]
        target[at, :] = jnp.where(inside, value, target[at, :])
        return 0

    lax.fori_loop(low // TILE, jnp.where(high > low, (high + TILE - 1) // TILE, low // TILE), tile, 0)


def window_start(counts_ref, plane, group):
    return before(counts_ref, plane * group) // (group * TILE)


def window_kernel(group, counts_ref, *rest):
    parts, window = rest[:group], rest[group]
    me = lax.axis_index("loader")
    member, plane = me % group, me // group
    tiles = parts[0].shape[0] // TILE
    start = window_start(counts_ref, plane, group)
    for k in range(group):
        source = plane * group + jnp.bitwise_xor(member, k)
        ranks = before(counts_ref, source)
        low = dealt(ranks, member, group)
        high = dealt(ranks + counts_ref[source], member, group)
        high = jnp.minimum(high, start * TILE + window.shape[0])
        copy_rows(low, high, parts[k], lambda t: t % tiles, window, lambda t: t - start)


def place_window(counts_ref, apart, group, rows, window, target):
    me = lax.axis_index("loader")
    member, plane = me % group, me // group
    origin = plane + apart
    planes = counts_ref.shape[0] // group
    bounded = jnp.minimum(origin, planes - 1)
    ranks = before(counts_ref, bounded * group)
    low = jnp.maximum(dealt(ranks, member, group), rows * plane)
    high = dealt(before(counts_ref, (bounded + 1) * group), member, group)
    high = jnp.where(origin < planes, jnp.minimum(high, rows * (plane + 1)), low)
    start = ranks // (group * TILE)
    first = rows // TILE * plane
    copy_rows(low, high, window, lambda t: t - start, target, lambda t: t - first)


def place_own(counts_ref, group, rows, parts, target):
    me = lax.axis_index("loader")
    member, plane = me % group, me // group
    tiles = parts[0].shape[0] // TILE
    first = rows // TILE * plane
    target[...] = jnp.zeros_like(target)
    for k in range(group):
        source = plane * group + jnp.bitwise_xor(member, k)
        ranks = before(counts_ref, source)
        low = jnp.maximum(dealt(ranks, member, group), rows * plane)
        high = jnp.minimum(dealt(ranks + counts_ref[source], member, group), rows * (plane + 1))
        copy_rows(low, high, parts[k], lambda t: t % tiles, target, lambda t: t - first)


def assemble_kernel(group, hops, counts_ref, *rest):
    parts, windows = rest[:group], rest[group : group + hops]
    outs, target = rest[group + hops : -1], rest[-1]
    rows = target.shape[0]
    place_own(counts_ref, group, rows, parts, target)
    for k in range(hops):
        place_window(counts_ref, k + 1, group, rows, windows[k], target)
    member = lax.axis_index("loader") % group
    share = rows // group
    for k in range(group):
        chunk = jnp.bitwise_xor(member, k) * share
        outs[k][...] = target[pl.ds(pl.multiple_of(chunk, TILE), share), :]


def own_kernel(group, counts_ref, *rest):
    place_own(counts_ref, group, rest[group].shape[0], rest[:group], rest[group])


def place_kernel(group, counts_ref, apart_ref, window, held, target):
    target[...] = held[...]
    place_window(counts_ref, apart_ref[0], group, target.shape[0], window, target)


def finish_kernel(group, *rest):
    left, right = rest[:group], rest[group : 2 * group]
    packed, scores = rest[2 * group :]
    width = left[0].shape[1]
    member = lax.axis_index("loader") % group
    tiles = left[0].shape[0] // TILE
    for k in range(group):
        owner = jnp.bitwise_xor(member, k)
        for t in range(tiles):
            at = pl.ds(pl.multiple_of((t * group + owner) * TILE, TILE), TILE)
            packed[at, :width] = left[k][t * TILE : (t + 1) * TILE, :]
            packed[at, width:] = right[k][t * TILE : (t + 1) * TILE, :]
    lanes = scores.shape[1]
    r = lax.broadcasted_iota(jnp.int32, (lanes, lanes), 0)
    c = lax.broadcasted_iota(jnp.int32, (lanes, lanes), 1)
    for s in range(scores.shape[0]):
        at = pl.ds(s * lanes, lanes)
        products = lax.dot_general(
            packed[at, :width], packed[at, width:], (((1,), (1,)), ((), ())), preferred_element_type=jnp.float32
        )
        own = jnp.where(r == c, products, 0.0)
        scores[s : s + 1, :] = jnp.sum(own, axis=0, keepdims=True) / width


def window_class_kernel(group, classes, counts_ref, class_ref):
    devices = counts_ref.shape[0]
    planes = devices // group
    turn = group * TILE
    edges = [jnp.int32(0)]
    for p in range(planes):
        edges.append(
            lax.fori_loop(p * group, (p + 1) * group, lambda s, total: total + counts_ref[s], edges[-1])
        )
    needed = []
    rows = classes[-1]
    for hop in range(1, planes):
        most = jnp.int32(0)
        for p in range(hop, planes):
            end = jnp.minimum(edges[p + 1], group * rows * (p - hop + 1))
            length = ((end + turn - 1) // turn - edges[p] // turn) * TILE
            most = jnp.maximum(most, jnp.where(end > edges[p], length, 0))
        needed.append(most)
    chosen = jnp.int32(len(classes) - 1)
    for index in reversed(range(len(classes) - 1)):
        fits = jnp.bool_(True)
        for hop in range(planes - 1):
            room = classes[index][hop] if hop < len(classes[index]) else 0
            fits = fits & (needed[hop] <= room)
        chosen = jnp.where(fits, jnp.int32(index), chosen)
    class_ref[0] = chosen


def all_counts_of(count, devices):
    me = lax.axis_index("loader")
    known = jnp.where(jnp.arange(devices, dtype=jnp.int32) == me, count, 0)
    for level in range((devices - 1).bit_length()):
        known = known + lax.ppermute(known, "loader", [(i, i ^ 1 << level) for i in range(devices)])
    return known


def exchange(parts, devices):
    received = [parts[0]]
    for k in range(1, len(parts)):
        received.append(lax.ppermute(parts[k], "loader", [(i, i ^ k) for i in range(devices)]))
    return received


def shards(image_embed, text_embed, keep_mask):
    rows, width = image_embed.shape
    devices = lax.axis_size("loader")
    group = group_of(devices)
    planes = devices // group
    share = rows // group
    dtype = image_embed.dtype
    part = jax.ShapeDtypeStruct((share, width), dtype)
    whole = jax.ShapeDtypeStruct((rows, width), dtype)

    marks = keep_mask.reshape(rows // BLOCK, BLOCK)
    sums = jnp.sum(marks, axis=1)
    counts = all_counts_of(jnp.sum(sums), devices)

    def pack(embed):
        return pl.pallas_call(
            functools.partial(pack_kernel, group),
            out_shape=[part] * group,
            in_specs=[SMEM, SMEM, VMEM, VMEM],
            out_specs=[VMEM] * group,
            scratch_shapes=[
                pltpu.VMEM((group, share, width), dtype),
                pltpu.VMEM(marks.shape, jnp.int32),
            ],
            name="pack",
        )(counts, sums, marks, embed)

    def window_of(parts, length):
        return pl.pallas_call(
            functools.partial(window_kernel, group),
            out_shape=jax.ShapeDtypeStruct((length, width), dtype),
            in_specs=[SMEM] + [VMEM] * group,
            out_specs=VMEM,
            name="window",
        )(counts, *parts)

    def assemble(parts, windows):
        return pl.pallas_call(
            functools.partial(assemble_kernel, group, len(windows)),
            out_shape=[part] * group,
            in_specs=[SMEM] + [VMEM] * (group + len(windows)),
            out_specs=[VMEM] * group,
            scratch_shapes=[pltpu.VMEM((rows, width), dtype)],
            name="assemble",
        )(counts, *parts, *windows)

    def down(window):
        return lax.ppermute(window, "loader", [(i, i - group) for i in range(group, devices)])

    def finish(left, right):
        packed, scores = pl.pallas_call(
            functools.partial(finish_kernel, group),
            out_shape=[
                jax.ShapeDtypeStruct((rows, 2 * width), dtype),
                jax.ShapeDtypeStruct((rows // 128, 128), jnp.float32),
            ],
            in_specs=[VMEM] * (2 * group),
            out_specs=[VMEM] * 2,
            name="finish",
        )(*left, *right)
        return packed, scores.reshape(rows)

    def fixed(lengths):
        def run(received, other):
            halves = [received, exchange(other, devices)]
            done = []
            for parts in halves:
                window = window_of(parts, lengths[0])
                windows = []
                for length in lengths:
                    window = down(window[:length])
                    windows.append(window)
                done.append(exchange(assemble(parts, windows), devices))
            return finish(*done)

        return run

    def general(received, other):
        halves = [received, exchange(other, devices)]
        member = lax.axis_index("loader") % group
        done = []
        for parts in halves:
            window = window_of(parts, rows + TILE)
            held = pl.pallas_call(
                functools.partial(own_kernel, group),
                out_shape=whole,
                in_specs=[SMEM] + [VMEM] * group,
                out_specs=VMEM,
                name="own",
            )(counts, *parts)

            def hop(k, state):
                window, held = state
                window = down(window)
                held = pl.pallas_call(
                    functools.partial(place_kernel, group),
                    out_shape=whole,
                    in_specs=[SMEM, SMEM, VMEM, VMEM],
                    out_specs=VMEM,
                    name="place",
                )(counts, k.reshape(1), window, held)
                return window, held

            _, held = lax.fori_loop(1, planes, hop, (window, held))
            chunks = held.reshape(group, share, width)
            parts = [lax.dynamic_index_in_dim(chunks, member ^ k, 0, keepdims=False) for k in range(group)]
            done.append(exchange(parts, devices))
        return finish(*done)

    lengths = [w for w in WINDOWS if w[0] <= rows and len(w) < planes]
    chosen = pl.pallas_call(
        functools.partial(window_class_kernel, group, tuple(lengths) + (rows,)),
        out_shape=jax.ShapeDtypeStruct((1,), jnp.int32),
        in_specs=[SMEM],
        out_specs=SMEM,
        name="choose",
    )(counts)
    received = exchange(pack(image_embed), devices)
    other = pack(text_embed)
    branches = [fixed(w) for w in lengths] + [general]
    return lax.switch(chosen[0], branches, received, other)


def solution(mesh):
    placed = (P("loader", None), P("loader", None), P("loader"))
    return jax.shard_map(
        shards,
        mesh=mesh,
        in_specs=placed,
        out_specs=(P("loader", None), P("loader")),
        check_vma=False,
    )
```

```python
import functools

import jax
import jax.numpy as jnp
from jax import lax
from jax.experimental import pallas as pl
from jax.experimental.pallas import tpu as pltpu
from jax.sharding import PartitionSpec as P


epsilon = 1e-06
TILE = 16
BLOCK = 256
SPLITS = (3, 6)
APART = (False, True, False)
WINDOWS = ((768, 704), (896, 832), (768, 768, 512), (1024, 1024, 256))

SMEM = pl.BlockSpec(memory_space=pltpu.SMEM)
VMEM = pl.BlockSpec(memory_space=pltpu.VMEM)


def group_of(devices):
    return 2 ** (devices.bit_length() // 2)


def dealt(rank, member, group):
    turn = group * TILE
    return rank // turn * TILE + jnp.clip(rank % turn - member * TILE, 0, TILE)


def pack_block(base, counts, ahead, block_of, packed, out):
    group = out.shape[0]
    tiles = out.shape[1] // TILE * group
    reach = BLOCK + TILE
    packed[...] = jnp.zeros_like(packed)
    r = lax.broadcasted_iota(jnp.int32, (reach, BLOCK), 0)
    position = base % TILE
    for b, count in enumerate(counts):
        at = pl.multiple_of(position // TILE * TILE, TILE)
        chosen = (ahead[b : b + 1, :] + position % TILE == r).astype(jnp.float32).astype(jnp.bfloat16)
        part = jnp.dot(chosen, block_of(b), preferred_element_type=jnp.float32).astype(jnp.bfloat16)
        packed[pl.ds(at, TILE), :] += part[:TILE]
        packed[pl.ds(at + TILE, BLOCK), :] = part[TILE:]
        position += count
    lap = tiles * TILE
    packed[:TILE, :] += packed[lap : lap + TILE, :]
    first = base // TILE % tiles

    def turn(t, _):
        for member in range(group):
            tile = t * group + member - first
            tile = jnp.where(tile < 0, tile + tiles, tile)
            out[member, pl.ds(pl.multiple_of(t * TILE, TILE), TILE), :] = packed[
                pl.ds(pl.multiple_of(tile * TILE, TILE), TILE), :
            ]
        return 0

    lax.fori_loop(0, tiles // group, turn, 0)


def kept_ahead(marks_ref):
    r = lax.broadcasted_iota(jnp.int32, (BLOCK, BLOCK), 0)
    c = lax.broadcasted_iota(jnp.int32, (BLOCK, BLOCK), 1)
    triangle = (r < c).astype(jnp.float32).astype(jnp.bfloat16)
    marks = marks_ref[...]
    ahead = jnp.dot(marks.astype(jnp.float32).astype(jnp.bfloat16), triangle, preferred_element_type=jnp.float32)
    return jnp.where(marks == 1, ahead.astype(jnp.int32), -2 * BLOCK)


def count_kernel(marks_ref, counts_ref):
    counts_ref[...] = jnp.full(counts_ref.shape, jnp.sum(marks_ref[...]), jnp.int32)


def first_pack_kernel(columns, all_ref, sums_ref, marks_ref, x_ref, out, edges, packed):
    devices = all_ref.shape[0]

    def step(s, total):
        edges[s] = total
        return total + all_ref[s, 0]

    edges[devices] = lax.fori_loop(0, devices, step, jnp.int32(0), unroll=8)
    base = edges[lax.axis_index("loader")]
    counts = [sums_ref[b] for b in range(marks_ref.shape[0])]
    pack_block(
        base, counts, kept_ahead(marks_ref), lambda b: x_ref[b * BLOCK : (b + 1) * BLOCK, columns], packed, out
    )


def pack_kernel(pieces, edges, sums_ref, marks_ref, left_ref, right_ref, *rest):
    outs, packed = rest[: len(pieces)], rest[len(pieces) :]
    base = edges[lax.axis_index("loader")]
    counts = [sums_ref[b] for b in range(marks_ref.shape[0])]
    ahead = kept_ahead(marks_ref)
    for p, (low, high) in enumerate(pieces):
        width = left_ref.shape[1]

        def block_of(b):
            rows = slice(b * BLOCK, (b + 1) * BLOCK)
            parts = []
            if low < width:
                parts.append(left_ref[rows, low : min(high, width)])
            if high > width:
                parts.append(right_ref[rows, max(low, width) - width : high - width])
            return parts[0] if len(parts) == 1 else jnp.concatenate(parts, axis=1)

        pack_block(base, counts, ahead, block_of, packed[p], outs[p])


def copy_rows(low, high, source, source_tile, target, target_tile):
    width = target.shape[-1]

    def ends(t):
        at = pl.ds(pl.multiple_of(target_tile(t) * TILE, TILE), TILE)
        return at, source[pl.ds(pl.multiple_of(source_tile(t) * TILE, TILE), TILE), :]

    def edge(t):
        at, value = ends(t)
        row = t * TILE + lax.broadcasted_iota(jnp.int32, (TILE, width), 0)
        target[at, :] = jnp.where((row >= low) & (row < high), value, target[at, :])

    def inner(t, _):
        at, value = ends(t)
        target[at, :] = value
        return 0

    first, last = low // TILE, high // TILE

    @pl.when((high > low) & (low % TILE != 0))
    def _():
        edge(first)

    lax.fori_loop((low + TILE - 1) // TILE, last, inner, 0)

    @pl.when((high > low) & (high % TILE != 0) & ((first != last) | (low % TILE == 0)))
    def _():
        edge(last)


def window_kernel(edges, parts, window):
    group, share = parts.shape[0], parts.shape[1]
    me = lax.axis_index("loader")
    member, plane = me % group, me // group
    tiles = share // TILE
    start = edges[plane * group] // (group * TILE)
    end = (start * TILE) + window.shape[0]

    def step(other, _):
        source = plane * group + other
        low = dealt(edges[source], member, group)
        high = jnp.minimum(dealt(edges[source + 1], member, group), end)
        copy_rows(low, high, parts.at[other], lambda t: t % tiles, window, lambda t: t - start)
        return 0

    lax.fori_loop(0, group, step, 0)


def place_window(edges, apart, group, rows, window, target):
    me = lax.axis_index("loader")
    member, plane = me % group, me // group
    origin = plane + apart
    planes = (edges.shape[0] - 1) // group
    bounded = jnp.minimum(origin, planes - 1)
    ranks = edges[bounded * group]
    low = jnp.maximum(dealt(ranks, member, group), rows * plane)
    high = dealt(edges[(bounded + 1) * group], member, group)
    high = jnp.where(origin < planes, jnp.minimum(high, rows * (plane + 1)), low)
    start = ranks // (group * TILE)
    first = rows // TILE * plane
    copy_rows(low, high, window, lambda t: t - start, target, lambda t: t - first)


def place_own(edges, parts, target):
    group, share = parts.shape[0], parts.shape[1]
    rows = target.shape[0]
    me = lax.axis_index("loader")
    member, plane = me % group, me // group
    tiles = share // TILE
    first = rows // TILE * plane
    target[...] = jnp.zeros_like(target)

    def step(other, _):
        source = plane * group + other
        low = jnp.maximum(dealt(edges[source], member, group), rows * plane)
        high = jnp.minimum(dealt(edges[source + 1], member, group), rows * (plane + 1))
        copy_rows(low, high, parts.at[other], lambda t: t % tiles, target, lambda t: t - first)
        return 0

    lax.fori_loop(0, group, step, 0)


def assemble_kernel(edges, parts, *rest):
    windows, target = rest[:-1], rest[-1]
    place_own(edges, parts, target)
    for k, window in enumerate(windows):
        place_window(edges, k + 1, parts.shape[0], target.shape[0], window, target)


def assemble_apart_kernel(hops, edges, parts, *rest):
    windows, outs, target = rest[:hops], rest[hops:-1], rest[-1]
    assemble_kernel(edges, parts, *windows, target)
    group, share = parts.shape[0], parts.shape[1]
    member = lax.axis_index("loader") % group
    for k in range(group):
        chunk = jnp.bitwise_xor(member, k) * share
        outs[k][...] = target[pl.ds(pl.multiple_of(chunk, TILE), share), :]


def place_kernel(group, edges, apart_ref, window, held, target):
    target[...] = held[...]
    place_window(edges, apart_ref[0], group, target.shape[0], window, target)


def finish_kernel(apart, *rest):
    parts, (packed, scores) = rest[:-2], rest[-2:]
    group = packed.shape[0] // (parts[0].shape[-2])
    member = lax.axis_index("loader") % group
    turn, width = group * TILE, packed.shape[1] // 2
    r = lax.broadcasted_iota(jnp.int32, (turn, turn), 0)
    c = lax.broadcasted_iota(jnp.int32, (turn, turn), 1)

    def step(t, _):
        source = pl.ds(pl.multiple_of(t * TILE, TILE), TILE)
        column, index = 0, 0
        for split in apart:
            width_here = parts[index].shape[-1]
            for k in range(group):
                owner = jnp.bitwise_xor(member, k) if split else k
                at = pl.ds(pl.multiple_of(t * turn + owner * TILE, TILE), TILE)
                tile = parts[index + k][source, :] if split else parts[index][k, source, :]
                packed[at, column : column + width_here] = tile
            column += width_here
            index += group if split else 1
        rows = pl.ds(pl.multiple_of(t * turn, turn), turn)
        units = []
        for low in (0, width):
            values = packed[rows, low : low + width].astype(jnp.float32)
            scale = lax.rsqrt(jnp.sum(values * values, axis=1, keepdims=True) / width + epsilon)
            unit = (values * scale).astype(packed.dtype)
            packed[rows, low : low + width] = unit
            units.append(unit)
        products = lax.dot_general(*units, (((1,), (1,)), ((), ())), preferred_element_type=jnp.float32)
        own = jnp.where(r == c, products, 0.0)
        scores[pl.ds(t, 1), :] = jnp.sum(own, axis=0, keepdims=True) / width
        return 0

    lax.fori_loop(0, packed.shape[0] // turn, step, 0, unroll=2)


def window_class_kernel(group, classes, edges, class_ref):
    planes = (edges.shape[0] - 1) // group
    turn = group * TILE
    needed = []
    rows = classes[-1]
    for hop in range(1, planes):
        most = jnp.int32(0)
        for p in range(hop, planes):
            start = edges[p * group]
            end = jnp.minimum(edges[(p + 1) * group], group * rows * (p - hop + 1))
            length = ((end + turn - 1) // turn - start // turn) * TILE
            most = jnp.maximum(most, jnp.where(end > start, length, 0))
        needed.append(most)
    chosen = jnp.int32(len(classes) - 1)
    for index in reversed(range(len(classes) - 1)):
        fits = jnp.bool_(True)
        for hop in range(planes - 1):
            room = classes[index][hop] if hop < len(classes[index]) else 0
            fits = fits & (needed[hop] <= room)
        chosen = jnp.where(fits, jnp.int32(index), chosen)
    class_ref[0] = chosen


def all_counts_of(marks, devices):
    counts = pl.pallas_call(
        count_kernel,
        out_shape=jax.ShapeDtypeStruct((devices, 128), jnp.int32),
        in_specs=[VMEM],
        out_specs=VMEM,
        name="count",
    )(marks)
    return lax.all_to_all(counts, "loader", 0, 0, tiled=True)


def exchange(parts, devices):
    group = parts.shape[0]
    planes = [[first + k for k in range(group)] for first in range(0, devices, group)]
    return lax.all_to_all(parts, "loader", 0, 0, axis_index_groups=planes, tiled=True)


def exchange_apart(parts, devices):
    received = [parts[0]]
    for k in range(1, len(parts)):
        received.append(lax.ppermute(parts[k], "loader", [(i, i ^ k) for i in range(devices)]))
    return received


def shards(image_embed, text_embed, keep_mask):
    rows, width = image_embed.shape
    devices = lax.axis_size("loader")
    group = group_of(devices)
    planes = devices // group
    share = rows // group
    dtype = image_embed.dtype
    turn = group * TILE
    bounds = [0] + [width * 2 * s // 8 for s in SPLITS] + [2 * width]
    widths = [high - low for low, high in zip(bounds, bounds[1:])]

    marks = keep_mask.reshape(rows // BLOCK, BLOCK)
    sums = jnp.sum(marks, axis=1)
    counts = all_counts_of(keep_mask, devices)

    def parts_of(chunk):
        return jax.ShapeDtypeStruct((group, share, widths[chunk]), dtype)

    def staging(chunk):
        return pltpu.VMEM((rows + BLOCK + 2 * TILE, widths[chunk]), dtype)

    first, edges = pl.pallas_call(
        functools.partial(first_pack_kernel, slice(bounds[0], bounds[1])),
        out_shape=[parts_of(0), jax.ShapeDtypeStruct((devices + 1,), jnp.int32)],
        in_specs=[SMEM, SMEM, VMEM, VMEM],
        out_specs=[VMEM, SMEM],
        scratch_shapes=[staging(0)],
        name="pack_first",
    )(counts, sums, marks, image_embed)

    def pack_rest():
        later = range(1, len(widths))
        return pl.pallas_call(
            functools.partial(pack_kernel, [(bounds[c], bounds[c + 1]) for c in later]),
            out_shape=[parts_of(c) for c in later],
            in_specs=[SMEM, SMEM, VMEM, VMEM, VMEM],
            out_specs=[VMEM] * len(later),
            scratch_shapes=[staging(c) for c in later],
            cost_estimate=pl.CostEstimate(flops=2**31, bytes_accessed=8 * rows * width, transcendentals=0),
            name="pack_rest",
        )(edges, sums, marks, image_embed, text_embed)

    def window_of(parts, length):
        return pl.pallas_call(
            window_kernel,
            out_shape=jax.ShapeDtypeStruct((length, parts.shape[2]), dtype),
            in_specs=[SMEM, VMEM],
            out_specs=VMEM,
            cost_estimate=pl.CostEstimate(flops=2**30, bytes_accessed=2 * rows * width, transcendentals=0),
            name="window",
        )(edges, parts)

    def assemble(parts, windows):
        return pl.pallas_call(
            assemble_kernel,
            out_shape=jax.ShapeDtypeStruct((rows, parts.shape[2]), dtype),
            in_specs=[SMEM] + [VMEM] * (1 + len(windows)),
            out_specs=VMEM,
            cost_estimate=pl.CostEstimate(flops=2**30, bytes_accessed=4 * rows * width, transcendentals=0),
            name="assemble",
        )(edges, parts, *windows)

    def assemble_apart(parts, windows):
        return pl.pallas_call(
            functools.partial(assemble_apart_kernel, len(windows)),
            out_shape=[jax.ShapeDtypeStruct((share, parts.shape[2]), dtype)] * group,
            in_specs=[SMEM] + [VMEM] * (1 + len(windows)),
            out_specs=[VMEM] * group,
            scratch_shapes=[pltpu.VMEM((rows, parts.shape[2]), dtype)],
            cost_estimate=pl.CostEstimate(flops=2**30, bytes_accessed=4 * rows * width, transcendentals=0),
            name="assemble_apart",
        )(edges, parts, *windows)

    def down(window):
        return lax.ppermute(window, "loader", [(i, i - group) for i in range(group, devices)])

    def gather(held):
        return exchange(held.reshape(group, share, held.shape[1]), devices)

    def fixed(lengths):
        def run(received, packed):
            chunks = [received]
            done = []
            for chunk in range(len(widths)):
                window = window_of(chunks[chunk], lengths[0])
                if chunk + 1 < len(widths):
                    window, following = lax.optimization_barrier((window, packed[chunk]))
                    chunks.append(exchange(following, devices))
                windows = []
                for length in lengths:
                    window = down(window[:length])
                    windows.append(window)
                held = (assemble_apart if APART[chunk] else assemble)(chunks[chunk], windows)
                done += exchange_apart(held, devices) if APART[chunk] else [gather(held)]
            return done

        return run

    def general(received, packed):
        parts = jnp.concatenate([received] + [exchange(part, devices) for part in packed], axis=2)
        window = window_of(parts, rows + TILE)
        held = assemble(parts, [])

        def hop(k, state):
            window, held = state
            window = down(window)
            held = pl.pallas_call(
                functools.partial(place_kernel, group),
                out_shape=jax.ShapeDtypeStruct(held.shape, dtype),
                in_specs=[SMEM, SMEM, VMEM, VMEM],
                out_specs=VMEM,
                name="place",
            )(edges, k.reshape(1), window, held)
            return window, held

        _, held = lax.fori_loop(1, planes, hop, (window, held))
        held = gather(held)
        member = lax.axis_index("loader") % group
        done = []
        for split, low, high in zip(APART, bounds, bounds[1:]):
            if split:
                done += [
                    lax.dynamic_index_in_dim(held, member ^ k, 0, keepdims=False)[:, low:high] for k in range(group)
                ]
            else:
                done.append(held[:, :, low:high])
        return done

    lengths = [w for w in WINDOWS if w[0] <= rows and len(w) < planes]
    chosen = pl.pallas_call(
        functools.partial(window_class_kernel, group, tuple(lengths) + (rows,)),
        out_shape=jax.ShapeDtypeStruct((1,), jnp.int32),
        in_specs=[SMEM],
        out_specs=SMEM,
        name="choose",
    )(edges)
    received = exchange(first, devices)
    branches = [fixed(w) for w in lengths] + [general]
    done = lax.switch(chosen[0], branches, received, pack_rest())
    packed_pairs, scores = pl.pallas_call(
        functools.partial(finish_kernel, APART),
        out_shape=[
            jax.ShapeDtypeStruct((rows, 2 * width), dtype),
            jax.ShapeDtypeStruct((rows // turn, turn), jnp.float32),
        ],
        in_specs=[VMEM] * len(done),
        out_specs=[VMEM] * 2,
        name="finish",
    )(*done)
    return packed_pairs, scores.reshape(rows)


def solution(mesh):
    placed = (P("loader", None), P("loader", None), P("loader"))
    return jax.shard_map(
        shards,
        mesh=mesh,
        in_specs=placed,
        out_specs=(P("loader", None), P("loader")),
        check_vma=False,
    )
```

```python
import functools

import jax
import jax.numpy as jnp
from jax import lax
from jax.experimental import pallas as pl
from jax.experimental.pallas import tpu as pltpu
from jax.sharding import PartitionSpec as P


epsilon = 1e-06
TILE = 16
BLOCK = 256
SPLITS = (3, 6)
APART = (False, True, False)
WINDOWS = ((768, 704), (896, 832), (768, 768, 512), (1024, 1024, 256))

SMEM = pl.BlockSpec(memory_space=pltpu.SMEM)
VMEM = pl.BlockSpec(memory_space=pltpu.VMEM)


def group_of(devices):
    return 2 ** (devices.bit_length() // 2)


def dealt(rank, member, group):
    turn = group * TILE
    return rank // turn * TILE + jnp.clip(rank % turn - member * TILE, 0, TILE)


def pack_block(base, counts, ahead, block_of, packed, out):
    group = out.shape[0]
    tiles = out.shape[1] // TILE * group
    reach = BLOCK + TILE
    packed[...] = jnp.zeros_like(packed)
    r = lax.broadcasted_iota(jnp.int32, (reach, BLOCK), 0)
    position = base % TILE
    for b, count in enumerate(counts):
        at = pl.multiple_of(position // TILE * TILE, TILE)
        chosen = (ahead[b : b + 1, :] + position % TILE == r).astype(jnp.float32).astype(jnp.bfloat16)
        part = jnp.dot(chosen, block_of(b), preferred_element_type=jnp.float32).astype(jnp.bfloat16)
        packed[pl.ds(at, TILE), :] += part[:TILE]
        packed[pl.ds(at + TILE, BLOCK), :] = part[TILE:]
        position += count
    lap = tiles * TILE
    packed[:TILE, :] += packed[lap : lap + TILE, :]
    first = base // TILE % tiles

    def turn(t, _):
        for member in range(group):
            tile = t * group + member - first
            tile = jnp.where(tile < 0, tile + tiles, tile)
            out[member, pl.ds(pl.multiple_of(t * TILE, TILE), TILE), :] = packed[
                pl.ds(pl.multiple_of(tile * TILE, TILE), TILE), :
            ]
        return 0

    lax.fori_loop(0, tiles // group, turn, 0)


def kept_ahead(marks_ref):
    r = lax.broadcasted_iota(jnp.int32, (BLOCK, BLOCK), 0)
    c = lax.broadcasted_iota(jnp.int32, (BLOCK, BLOCK), 1)
    triangle = (r < c).astype(jnp.float32).astype(jnp.bfloat16)
    marks = marks_ref[...]
    ahead = jnp.dot(marks.astype(jnp.float32).astype(jnp.bfloat16), triangle, preferred_element_type=jnp.float32)
    return jnp.where(marks == 1, ahead.astype(jnp.int32), -2 * BLOCK)


def count_kernel(marks_ref, counts_ref):
    counts_ref[...] = jnp.full(counts_ref.shape, jnp.sum(marks_ref[...]), jnp.int32)


def first_pack_kernel(columns, all_ref, sums_ref, marks_ref, x_ref, out, edges, packed):
    devices = all_ref.shape[0]

    def step(s, total):
        edges[s] = total
        return total + all_ref[s, 0]

    edges[devices] = lax.fori_loop(0, devices, step, jnp.int32(0), unroll=8)
    base = edges[lax.axis_index("loader")]
    counts = [sums_ref[b] for b in range(marks_ref.shape[0])]
    pack_block(
        base, counts, kept_ahead(marks_ref), lambda b: x_ref[b * BLOCK : (b + 1) * BLOCK, columns], packed, out
    )


def pack_kernel(pieces, edges, sums_ref, marks_ref, left_ref, right_ref, *rest):
    outs, packed = rest[: len(pieces)], rest[len(pieces) :]
    base = edges[lax.axis_index("loader")]
    counts = [sums_ref[b] for b in range(marks_ref.shape[0])]
    ahead = kept_ahead(marks_ref)
    for p, (low, high) in enumerate(pieces):
        width = left_ref.shape[1]

        def block_of(b):
            rows = slice(b * BLOCK, (b + 1) * BLOCK)
            parts = []
            if low < width:
                parts.append(left_ref[rows, low : min(high, width)])
            if high > width:
                parts.append(right_ref[rows, max(low, width) - width : high - width])
            return parts[0] if len(parts) == 1 else jnp.concatenate(parts, axis=1)

        pack_block(base, counts, ahead, block_of, packed[p], outs[p])


def copy_rows(low, high, source, source_tile, target, target_tile):
    width = target.shape[-1]

    def ends(t):
        at = pl.ds(pl.multiple_of(target_tile(t) * TILE, TILE), TILE)
        return at, source[pl.ds(pl.multiple_of(source_tile(t) * TILE, TILE), TILE), :]

    def edge(t):
        at, value = ends(t)
        row = t * TILE + lax.broadcasted_iota(jnp.int32, (TILE, width), 0)
        target[at, :] = jnp.where((row >= low) & (row < high), value, target[at, :])

    def inner(t, _):
        at, value = ends(t)
        target[at, :] = value
        return 0

    first, last = low // TILE, high // TILE

    @pl.when((high > low) & (low % TILE != 0))
    def _():
        edge(first)

    lax.fori_loop((low + TILE - 1) // TILE, last, inner, 0)

    @pl.when((high > low) & (high % TILE != 0) & ((first != last) | (low % TILE == 0)))
    def _():
        edge(last)


def window_kernel(edges, parts, window):
    group, share = parts.shape[0], parts.shape[1]
    me = lax.axis_index("loader")
    member, plane = me % group, me // group
    tiles = share // TILE
    start = edges[plane * group] // (group * TILE)
    end = (start * TILE) + window.shape[0]

    def step(other, _):
        source = plane * group + other
        low = dealt(edges[source], member, group)
        high = jnp.minimum(dealt(edges[source + 1], member, group), end)
        copy_rows(low, high, parts.at[other], lambda t: t % tiles, window, lambda t: t - start)
        return 0

    lax.fori_loop(0, group, step, 0)


def place_window(edges, apart, group, rows, window, target):
    me = lax.axis_index("loader")
    member, plane = me % group, me // group
    origin = plane + apart
    planes = (edges.shape[0] - 1) // group
    bounded = jnp.minimum(origin, planes - 1)
    ranks = edges[bounded * group]
    low = jnp.maximum(dealt(ranks, member, group), rows * plane)
    high = dealt(edges[(bounded + 1) * group], member, group)
    high = jnp.where(origin < planes, jnp.minimum(high, rows * (plane + 1)), low)
    start = ranks // (group * TILE)
    first = rows // TILE * plane
    copy_rows(low, high, window, lambda t: t - start, target, lambda t: t - first)


def place_own(edges, parts, target):
    group, share = parts.shape[0], parts.shape[1]
    rows = target.shape[0]
    me = lax.axis_index("loader")
    member, plane = me % group, me // group
    tiles = share // TILE
    first = rows // TILE * plane
    target[...] = jnp.zeros_like(target)

    def step(other, _):
        source = plane * group + other
        low = jnp.maximum(dealt(edges[source], member, group), rows * plane)
        high = jnp.minimum(dealt(edges[source + 1], member, group), rows * (plane + 1))
        copy_rows(low, high, parts.at[other], lambda t: t % tiles, target, lambda t: t - first)
        return 0

    lax.fori_loop(0, group, step, 0)


def assemble_kernel(edges, parts, *rest):
    windows, target = rest[:-1], rest[-1]
    place_own(edges, parts, target)
    for k, window in enumerate(windows):
        place_window(edges, k + 1, parts.shape[0], target.shape[0], window, target)


def assemble_apart_kernel(hops, edges, parts, *rest):
    windows, outs, target = rest[:hops], rest[hops:-1], rest[-1]
    assemble_kernel(edges, parts, *windows, target)
    group, share = parts.shape[0], parts.shape[1]
    member = lax.axis_index("loader") % group
    for k in range(group):
        chunk = jnp.bitwise_xor(member, k) * share
        outs[k][...] = target[pl.ds(pl.multiple_of(chunk, TILE), share), :]


def place_kernel(group, edges, apart_ref, window, held, target):
    target[...] = held[...]
    place_window(edges, apart_ref[0], group, target.shape[0], window, target)


def unit_of(values, dtype):
    values = values.astype(jnp.float32)
    scale = lax.rsqrt(jnp.sum(values * values, axis=1, keepdims=True) / values.shape[1] + epsilon)
    return (values * scale).astype(dtype)


def stage_kernel(apart, width, *rest):
    parts, staged = rest[:-1], rest[-1]
    group = staged.shape[0] // parts[0].shape[-2]
    member = lax.axis_index("loader") % group
    turn = group * TILE

    def step(t, _):
        source = pl.ds(pl.multiple_of(t * TILE, TILE), TILE)
        column, index = 0, 0
        for split in apart[:-1]:
            width_here = parts[index].shape[-1]
            for k in range(group):
                owner = jnp.bitwise_xor(member, k) if split else k
                at = pl.ds(pl.multiple_of(t * turn + owner * TILE, TILE), TILE)
                tile = parts[index + k][source, :] if split else parts[index][k, source, :]
                staged[at, column : column + width_here] = tile
            column += width_here
            index += group if split else 1
        rows = pl.ds(pl.multiple_of(t * turn, turn), turn)
        staged[rows, :width] = unit_of(staged[rows, :width], staged.dtype)
        return 0

    lax.fori_loop(0, staged.shape[0] // turn, step, 0, unroll=2)


def finish_kernel(staged, last, packed, scores):
    group, width = last.shape[0], packed.shape[1] // 2
    turn = group * TILE
    r = lax.broadcasted_iota(jnp.int32, (turn, turn), 0)
    c = lax.broadcasted_iota(jnp.int32, (turn, turn), 1)

    def step(t, _):
        source = pl.ds(pl.multiple_of(t * TILE, TILE), TILE)
        rows = pl.ds(pl.multiple_of(t * turn, turn), turn)
        tiles = jnp.concatenate([last[owner, source, :] for owner in range(group)], axis=0)
        right = unit_of(jnp.concatenate([staged[rows, width:], tiles], axis=1), packed.dtype)
        left = staged[rows, :width]
        packed[rows, :width] = left
        packed[rows, width:] = right
        products = lax.dot_general(left, right, (((1,), (1,)), ((), ())), preferred_element_type=jnp.float32)
        own = jnp.where(r == c, products, 0.0)
        scores[pl.ds(t, 1), :] = jnp.sum(own, axis=0, keepdims=True) / width
        return 0

    lax.fori_loop(0, packed.shape[0] // turn, step, 0, unroll=2)


def window_class_kernel(group, classes, edges, class_ref):
    planes = (edges.shape[0] - 1) // group
    turn = group * TILE
    needed = []
    rows = classes[-1]
    for hop in range(1, planes):
        most = jnp.int32(0)
        for p in range(hop, planes):
            start = edges[p * group]
            end = jnp.minimum(edges[(p + 1) * group], group * rows * (p - hop + 1))
            length = ((end + turn - 1) // turn - start // turn) * TILE
            most = jnp.maximum(most, jnp.where(end > start, length, 0))
        needed.append(most)
    chosen = jnp.int32(len(classes) - 1)
    for index in reversed(range(len(classes) - 1)):
        fits = jnp.bool_(True)
        for hop in range(planes - 1):
            room = classes[index][hop] if hop < len(classes[index]) else 0
            fits = fits & (needed[hop] <= room)
        chosen = jnp.where(fits, jnp.int32(index), chosen)
    class_ref[0] = chosen


def all_counts_of(marks, devices):
    counts = pl.pallas_call(
        count_kernel,
        out_shape=jax.ShapeDtypeStruct((devices, 128), jnp.int32),
        in_specs=[VMEM],
        out_specs=VMEM,
        name="count",
    )(marks)
    return lax.all_to_all(counts, "loader", 0, 0, tiled=True)


def exchange(parts, devices):
    group = parts.shape[0]
    planes = [[first + k for k in range(group)] for first in range(0, devices, group)]
    return lax.all_to_all(parts, "loader", 0, 0, axis_index_groups=planes, tiled=True)


def exchange_apart(parts, devices):
    received = [parts[0]]
    for k in range(1, len(parts)):
        received.append(lax.ppermute(parts[k], "loader", [(i, i ^ k) for i in range(devices)]))
    return received


def shards(image_embed, text_embed, keep_mask):
    rows, width = image_embed.shape
    devices = lax.axis_size("loader")
    group = group_of(devices)
    planes = devices // group
    share = rows // group
    dtype = image_embed.dtype
    turn = group * TILE
    bounds = [0] + [width * 2 * s // 8 for s in SPLITS] + [2 * width]
    widths = [high - low for low, high in zip(bounds, bounds[1:])]

    marks = keep_mask.reshape(rows // BLOCK, BLOCK)
    sums = jnp.sum(marks, axis=1)
    counts = all_counts_of(keep_mask, devices)

    def parts_of(chunk):
        return jax.ShapeDtypeStruct((group, share, widths[chunk]), dtype)

    def staging(chunk):
        return pltpu.VMEM((rows + BLOCK + 2 * TILE, widths[chunk]), dtype)

    first, edges = pl.pallas_call(
        functools.partial(first_pack_kernel, slice(bounds[0], bounds[1])),
        out_shape=[parts_of(0), jax.ShapeDtypeStruct((devices + 1,), jnp.int32)],
        in_specs=[SMEM, SMEM, VMEM, VMEM],
        out_specs=[VMEM, SMEM],
        scratch_shapes=[staging(0)],
        name="pack_first",
    )(counts, sums, marks, image_embed)

    def pack_rest():
        later = range(1, len(widths))
        return pl.pallas_call(
            functools.partial(pack_kernel, [(bounds[c], bounds[c + 1]) for c in later]),
            out_shape=[parts_of(c) for c in later],
            in_specs=[SMEM, SMEM, VMEM, VMEM, VMEM],
            out_specs=[VMEM] * len(later),
            scratch_shapes=[staging(c) for c in later],
            cost_estimate=pl.CostEstimate(flops=2**31, bytes_accessed=8 * rows * width, transcendentals=0),
            name="pack_rest",
        )(edges, sums, marks, image_embed, text_embed)

    def window_of(parts, length):
        return pl.pallas_call(
            window_kernel,
            out_shape=jax.ShapeDtypeStruct((length, parts.shape[2]), dtype),
            in_specs=[SMEM, VMEM],
            out_specs=VMEM,
            cost_estimate=pl.CostEstimate(flops=2**30, bytes_accessed=2 * rows * width, transcendentals=0),
            name="window",
        )(edges, parts)

    def assemble(parts, windows):
        return pl.pallas_call(
            assemble_kernel,
            out_shape=jax.ShapeDtypeStruct((rows, parts.shape[2]), dtype),
            in_specs=[SMEM] + [VMEM] * (1 + len(windows)),
            out_specs=VMEM,
            cost_estimate=pl.CostEstimate(flops=2**30, bytes_accessed=4 * rows * width, transcendentals=0),
            name="assemble",
        )(edges, parts, *windows)

    def assemble_apart(parts, windows):
        return pl.pallas_call(
            functools.partial(assemble_apart_kernel, len(windows)),
            out_shape=[jax.ShapeDtypeStruct((share, parts.shape[2]), dtype)] * group,
            in_specs=[SMEM] + [VMEM] * (1 + len(windows)),
            out_specs=[VMEM] * group,
            scratch_shapes=[pltpu.VMEM((rows, parts.shape[2]), dtype)],
            cost_estimate=pl.CostEstimate(flops=2**30, bytes_accessed=4 * rows * width, transcendentals=0),
            name="assemble_apart",
        )(edges, parts, *windows)

    def down(window):
        return lax.ppermute(window, "loader", [(i, i - group) for i in range(group, devices)])

    def gather(held):
        return exchange(held.reshape(group, share, held.shape[1]), devices)

    def fixed(lengths):
        def run(received, packed):
            chunks = [received]
            done = []
            for chunk in range(len(widths)):
                window = window_of(chunks[chunk], lengths[0])
                if chunk + 1 < len(widths):
                    window, following = lax.optimization_barrier((window, packed[chunk]))
                    chunks.append(exchange(following, devices))
                windows = []
                for length in lengths:
                    window = down(window[:length])
                    windows.append(window)
                held = (assemble_apart if APART[chunk] else assemble)(chunks[chunk], windows)
                if chunk + 1 == len(widths):
                    return done, held
                done += exchange_apart(held, devices) if APART[chunk] else [gather(held)]

        return run

    def general(received, packed):
        parts = jnp.concatenate([received] + [exchange(part, devices) for part in packed], axis=2)
        window = window_of(parts, rows + TILE)
        held = assemble(parts, [])

        def hop(k, state):
            window, held = state
            window = down(window)
            held = pl.pallas_call(
                functools.partial(place_kernel, group),
                out_shape=jax.ShapeDtypeStruct(held.shape, dtype),
                in_specs=[SMEM, SMEM, VMEM, VMEM],
                out_specs=VMEM,
                name="place",
            )(edges, k.reshape(1), window, held)
            return window, held

        _, held = lax.fori_loop(1, planes, hop, (window, held))
        early = gather(held[:, : bounds[-2]])
        member = lax.axis_index("loader") % group
        done = []
        for split, low, high in zip(APART, bounds, bounds[1:-1]):
            if split:
                done += [
                    lax.dynamic_index_in_dim(early, member ^ k, 0, keepdims=False)[:, low:high] for k in range(group)
                ]
            else:
                done.append(early[:, :, low:high])
        return done, held[:, bounds[-2] :]

    lengths = [w for w in WINDOWS if w[0] <= rows and len(w) < planes]
    chosen = pl.pallas_call(
        functools.partial(window_class_kernel, group, tuple(lengths) + (rows,)),
        out_shape=jax.ShapeDtypeStruct((1,), jnp.int32),
        in_specs=[SMEM],
        out_specs=SMEM,
        name="choose",
    )(edges)
    received = exchange(first, devices)
    branches = [fixed(w) for w in lengths] + [general]
    done, held = lax.switch(chosen[0], branches, received, pack_rest())
    last = gather(held)
    staged = pl.pallas_call(
        functools.partial(stage_kernel, APART, width),
        out_shape=jax.ShapeDtypeStruct((rows, bounds[-2]), dtype),
        in_specs=[VMEM] * len(done),
        out_specs=VMEM,
        cost_estimate=pl.CostEstimate(flops=2**31, bytes_accessed=8 * rows * width, transcendentals=rows),
        name="stage",
    )(*done)
    packed_pairs, scores = pl.pallas_call(
        finish_kernel,
        out_shape=[
            jax.ShapeDtypeStruct((rows, 2 * width), dtype),
            jax.ShapeDtypeStruct((rows // turn, turn), jnp.float32),
        ],
        in_specs=[VMEM] * 2,
        out_specs=[VMEM] * 2,
        name="finish",
    )(staged, last)
    return packed_pairs, scores.reshape(rows)


def solution(mesh):
    placed = (P("loader", None), P("loader", None), P("loader"))
    return jax.shard_map(
        shards,
        mesh=mesh,
        in_specs=placed,
        out_specs=(P("loader", None), P("loader")),
        check_vma=False,
    )
```
